32 devices in a mesh: mod: 2 (over y), dp: 16 (over z, x, core).
Axes of the slice: x: 2, y: 2, z: 4, core: 2. Of those that a mesh axis runs over, the one named last changes fastest.
Arguments:
- image_pooled: bfloat16 [640, 1024], P('dp'), may hold values from -6 to 6
- text_pooled: bfloat16 [640, 768], P('dp'), may hold values from -6 to 6
- image_gain: float32 [1024], replicated, may hold values from 0.25 to 1.75
- text_gain: float32 [768], replicated, may hold values from 0.25 to 1.75
- image_proj: bfloat16 [1024, 768], replicated, may hold values from -0.1875 to 0.1875
- text_proj: bfloat16 [768, 768], replicated, may hold values from -0.21875 to 0.21875
- logit_scale: float32 [1], replicated, may hold values from 10 to 100
- pair_index: int32 [2, 640], P('mod', 'dp'), may hold values from 0 to 639, as said below
Outputs:
- loss_value: float32 [], replicated
- embed_grad: float32 [2, 640, 768], P('mod', 'dp')
The draws below stay inside these ranges and needn't reach their ends.
Inputs may be any that keep to these rules, and one draw needn't show every extreme that they name: `pair_index`: row 0 is a permutation of 0 to 639 and row 1 is its inverse permutation.
All inputs are finite; a program needn't handle non-finite values.
Results may differ from the reference program's by a relative error of at most 0.0041.
Values may be sent and summed in bfloat16 or wider, within the bound.
No kernel may reach another device: no remote copies, remote signals or barrier semaphores. Data moves between devices by JAX's collectives and lax.ppermute only.
A program may use at most 128 MiB of HBM per device.

```python
import math
import jax
import jax.numpy as jnp
from jax import lax

DI = 1024
DT = 768
EMBED = 768
ROWS = 40
BATCH = 640
N_DP = 16


def draw_pair_index(key, part):
    forward = jax.random.permutation(jax.random.fold_in(key, 11), BATCH).astype(jnp.int32)
    inverse = jnp.argsort(forward, stable=True).astype(jnp.int32)
    return jnp.stack([forward, inverse])


def shard_levels(rng, extent, pieces, smallest, largest):
    def one(dim, blocks):
        heights = jax.random.uniform(jax.random.fold_in(jax.random.fold_in(rng, 6), dim), (blocks,), jnp.float32, smallest / len(pieces), largest / len(pieces))
        return jnp.repeat(jnp.exp(heights), extent[dim] // blocks).reshape((-1,) + (1,) * (len(extent) - dim - 1))

    level = one(*pieces[0])
    for cut in pieces[1:]:
        level = level * one(*cut)
    return level


def noise(key, shape, spread, limit, split=(), held_as=jnp.bfloat16):
    entries = spread * jax.random.normal(key, shape, jnp.float32)
    if split:
        entries = entries * shard_levels(key, shape, split, -0.22, 0.18)
    return jnp.clip(entries, -limit, limit).astype(held_as)


def setup_inputs(seed: int = 0) -> dict:
    streams_of = jax.random.split(jax.random.key(seed), 9)
    return {
        "image_pooled": noise(streams_of[0], (BATCH, DI), 1.0, 6.0, ((0, 16),)),
        "text_pooled": noise(streams_of[1], (BATCH, DT), 1.0, 6.0, ((0, 16),)),
        "image_gain": jnp.clip(1.0 + 0.15 * jax.random.normal(streams_of[2], (DI,), jnp.float32), 0.25, 1.75),
        "text_gain": jnp.clip(1.0 + 0.15 * jax.random.normal(streams_of[3], (DT,), jnp.float32), 0.25, 1.75),
        "image_proj": noise(streams_of[4], (DI, EMBED), DI ** -0.5, 0.1875),
        "text_proj": noise(streams_of[5], (DT, EMBED), DT ** -0.5, 0.21875),
        "logit_scale": jnp.clip(jnp.exp(jax.random.uniform(streams_of[6], (1,), jnp.float32, math.log(10.0), math.log(100.0))), 10.0, 100.0),
        "pair_index": draw_pair_index(jax.random.fold_in(streams_of[8], 71), 0),
    }


def normalize_project(pooled, gain, weight):
    features = pooled.astype(jnp.float32)
    centered = features - lax.optimization_barrier(jnp.mean(features, axis=-1, keepdims=True))
    variance = lax.optimization_barrier(jnp.mean(centered * centered, axis=-1, keepdims=True))
    normalized = (centered * lax.rsqrt(variance + 1e-05) * gain).astype(jnp.bfloat16)
    return jnp.dot(normalized, weight, preferred_element_type=jnp.float32)

def unitize(embedded):
    lengths = jnp.sqrt(lax.optimization_barrier(jnp.sum(embedded * embedded, axis=-1, keepdims=True)) + 1e-06)
    return (embedded / lengths, lengths)

def similarity(left_rows, right_rows, scale_value):
    return scale_value * lax.dot_general(left_rows, right_rows, (((1,), (1,)), ((), ())), preferred_element_type=jnp.float32)

def lse_pass(own_half, other_half, partners, scale_value):
    width = own_half.shape[1]

    def one_block(inputs):
        block_rows, block_pairs = inputs
        score_block = similarity(block_rows, other_half, scale_value)
        running_max = lax.optimization_barrier(jnp.max(score_block, axis=1))
        block_lse = running_max + jnp.log(lax.optimization_barrier(jnp.sum(jnp.exp(score_block - running_max[:, None]), axis=1)))
        columns = lax.broadcasted_iota(jnp.int32, score_block.shape, 1)
        matched = columns == block_pairs[:, None]
        block_diag = lax.optimization_barrier(jnp.sum(jnp.where(matched, score_block, 0.0), axis=1))
        return (block_lse, block_diag)
    lse_blocks, diag_blocks = lax.map(one_block, (own_half.reshape(N_DP, ROWS, width), partners.reshape(N_DP, ROWS)))
    return (lse_blocks.reshape(-1), diag_blocks.reshape(-1))

def grad_pass(own_half, other_half, own_lse, other_lse, partners, scale_value, unit_rows, lengths):
    width = own_half.shape[1]
    batch_total = own_half.shape[0]

    def one_block(inputs):
        block_rows, block_lse, block_pairs, block_unit, block_len = inputs
        score_block = similarity(block_rows, other_half, scale_value)
        columns = lax.broadcasted_iota(jnp.int32, score_block.shape, 1)
        matched = (columns == block_pairs[:, None]).astype(jnp.float32)
        pair_weight = (jnp.exp(score_block - block_lse[:, None]) + jnp.exp(score_block - other_lse[None, :]) - 2.0 * matched).astype(jnp.bfloat16)
        unit_grad = scale_value / (2.0 * batch_total) * jnp.dot(pair_weight, other_half, preferred_element_type=jnp.float32)
        return (unit_grad - block_unit * lax.optimization_barrier(jnp.sum(block_unit * unit_grad, axis=-1, keepdims=True))) / block_len
    grad_blocks = lax.map(one_block, (own_half.reshape(N_DP, ROWS, width), own_lse.reshape(N_DP, ROWS), partners.reshape(N_DP, ROWS), unit_rows.reshape(N_DP, ROWS, width), lengths.reshape(N_DP, ROWS, 1)))
    return grad_blocks.reshape(batch_total, width)

def reference(image_pooled, text_pooled, image_gain, text_gain, image_proj, text_proj, logit_scale, pair_index):
    image_unit, image_len = unitize(normalize_project(image_pooled, image_gain, image_proj))
    text_unit, text_len = unitize(normalize_project(text_pooled, text_gain, text_proj))
    image_half = image_unit.astype(jnp.bfloat16)
    text_half = text_unit.astype(jnp.bfloat16)
    scale_value = logit_scale[0]
    image_lse, image_diag = lse_pass(image_half, text_half, pair_index[0], scale_value)
    text_lse, text_diag = lse_pass(text_half, image_half, pair_index[1], scale_value)
    batch_total = image_half.shape[0]
    loss_value = (jnp.sum(image_lse - image_diag) + jnp.sum(text_lse - text_diag)) / (2.0 * batch_total)
    image_grad = grad_pass(image_half, text_half, image_lse, text_lse, pair_index[0], scale_value, image_unit, image_len)
    text_grad = grad_pass(text_half, image_half, text_lse, image_lse, pair_index[1], scale_value, text_unit, text_len)
    return (loss_value, jnp.stack([image_grad, text_grad]))
```

```python
import jax
import jax.numpy as jnp
import numpy as np
from jax import lax
from jax.sharding import PartitionSpec as P

LANES = 128
SCORE_BYTES = 2**24


def closed_path(mesh):
    places = [getattr(d, "coords", None) for d in mesh.devices[0]]
    natural = list(range(len(places)))
    if any(p is None for p in places):
        return natural
    chips = {}
    for i, p in enumerate(places):
        chips.setdefault(tuple(p), []).append(i)
    span = [sorted({c[k] for c in chips}) for k in range(3)]
    wide = [k for k in range(3) if len(span[k]) > 1]
    if len(wide) != 2 or len(chips) != len(span[wide[0]]) * len(span[wide[1]]):
        return natural
    short, long = sorted(wide, key=lambda k: len(span[k]))
    if len(span[short]) != 2:
        return natural
    by = {(c[short], c[long]): v for c, v in chips.items()}
    there = [by[span[short][0], z] for z in span[long]]
    back = [by[span[short][1], z] for z in reversed(span[long])]
    return [i for cores in there + back for i in cores]


def from_partner(x, axis, bit):
    return lax.ppermute(x, axis, [(i, i ^ 1 << bit) for i in range(lax.axis_size(axis))])


def normalize_project(pooled, gain, weight):
    features = pooled.astype(jnp.float32)
    centered = features - jnp.mean(features, axis=-1, keepdims=True)
    variance = jnp.mean(centered * centered, axis=-1, keepdims=True)
    normalized = (centered * lax.rsqrt(variance + 1e-05) * gain).astype(jnp.bfloat16)
    return jnp.dot(normalized, weight, preferred_element_type=jnp.float32)


def unitize(embedded):
    lengths = jnp.sqrt(jnp.sum(embedded * embedded, axis=-1, keepdims=True) + 1e-06)
    return (embedded / lengths, lengths)


def similarity(left_rows, right_rows, scale_value):
    return scale_value * lax.dot_general(
        left_rows, right_rows, (((1,), (1,)), ((), ())), preferred_element_type=jnp.float32
    )


def log_sum_exp(scores, axis):
    top = jnp.max(scores, axis=axis)
    return top + jnp.log(jnp.sum(jnp.exp(scores - jnp.expand_dims(top, axis)), axis=axis))


def gather_both(
    order, image_pooled, text_pooled, image_gain, text_gain, image_proj, text_proj, logit_scale, pair_index
):
    is_image = lax.axis_index("mod") == 0
    image_unit, image_len = unitize(normalize_project(image_pooled, image_gain, image_proj))
    text_unit, text_len = unitize(normalize_project(text_pooled, text_gain, text_proj))
    unit_rows = jnp.where(is_image, image_unit, text_unit)
    other_rows = jnp.where(is_image, text_unit, image_unit)
    lengths = jnp.where(is_image, image_len, text_len)
    scale_value = logit_scale[0]
    row_count, width = unit_rows.shape
    batch_total = row_count * lax.axis_size("dp")
    pairs = pair_index[0][:, None]
    lane = lax.broadcasted_iota(jnp.int32, (row_count, LANES), 1)
    digits = jnp.where(lane == 0, pairs // LANES, jnp.where(lane == 1, pairs % LANES, 0))
    sent = jnp.concatenate(
        [
            unit_rows.astype(jnp.bfloat16).astype(jnp.float16),
            other_rows.astype(jnp.bfloat16).astype(jnp.float16),
            digits.astype(jnp.float16),
        ],
        axis=1,
    )
    every = lax.all_gather(sent, "dp", axis=0, tiled=True, axis_index_groups=[order])
    own_all = every[:, :width].astype(jnp.bfloat16)
    other_all = every[:, width : 2 * width].astype(jnp.bfloat16)
    digits_all = every[:, 2 * width : 2 * width + 2].astype(jnp.int32)
    pairs_all = digits_all[:, 0] * LANES + digits_all[:, 1]
    sample_of = jnp.asarray(
        np.concatenate([np.arange(row_count) + i * row_count for i in order]), jnp.int32
    )
    place = jnp.asarray(np.argsort(order), jnp.int32)[lax.axis_index("dp")] * row_count
    scores_all = similarity(own_all, other_all, scale_value)
    row_lse = log_sum_exp(scores_all, 1)
    col_lse = log_sum_exp(scores_all, 0)
    hit = sample_of[None, :] == pairs_all[:, None]
    diagonal = jnp.sum(jnp.where(hit, scores_all, 0.0))
    loss_value = (jnp.sum(row_lse) + jnp.sum(col_lse) - 2.0 * diagonal) / (2.0 * batch_total)
    scores = lax.dynamic_slice_in_dim(scores_all, place, row_count)
    own_lse = lax.dynamic_slice_in_dim(row_lse, place, row_count)
    matched = sample_of[None, :] == pairs
    pair_weight = (
        jnp.exp(scores - own_lse[:, None])
        + jnp.exp(scores - col_lse[None, :])
        - 2.0 * matched.astype(jnp.float32)
    ).astype(jnp.bfloat16)
    unit_grad = (
        scale_value
        / (2.0 * batch_total)
        * jnp.dot(pair_weight, other_all, preferred_element_type=jnp.float32)
    )
    embed_grad = (
        unit_grad - unit_rows * jnp.sum(unit_rows * unit_grad, axis=-1, keepdims=True)
    ) / lengths
    return (loss_value, embed_grad[None])


def gather_one(
    image_pooled, text_pooled, image_gain, text_gain, image_proj, text_proj, logit_scale, pair_index
):
    module_index = lax.axis_index("mod")
    embedded = lax.cond(
        module_index == 0,
        lambda: normalize_project(image_pooled, image_gain, image_proj),
        lambda: normalize_project(text_pooled, text_gain, text_proj),
    )
    unit_rows, lengths = unitize(embedded)
    unit_half = unit_rows.astype(jnp.bfloat16)
    mirror_rows = from_partner(unit_half, "mod", 0)
    scale_value = logit_scale[0]
    row_count = unit_rows.shape[0]
    batch_total = row_count * lax.axis_size("dp")
    gathered = lax.all_gather(mirror_rows, "dp", axis=0, tiled=True)
    scores = similarity(unit_half, gathered, scale_value)
    own_lse = log_sum_exp(scores, 1)
    columns = lax.broadcasted_iota(jnp.int32, (row_count, batch_total), 1)
    matched = columns == pair_index[0][:, None]
    diagonal = jnp.sum(jnp.where(matched, scores, 0.0), axis=1)
    every_lse, every_diag = (
        lax.all_gather(own_lse, ("mod", "dp"), axis=0, tiled=True),
        lax.all_gather(diagonal, ("mod", "dp"), axis=0, tiled=True),
    )
    other_lse = lax.dynamic_slice_in_dim(every_lse, (1 - module_index) * batch_total, batch_total)
    loss_value = (jnp.sum(every_lse) - jnp.sum(every_diag)) / (2.0 * batch_total)
    pair_weight = (
        jnp.exp(scores - own_lse[:, None])
        + jnp.exp(scores - other_lse[None, :])
        - 2.0 * matched.astype(jnp.float32)
    ).astype(jnp.bfloat16)
    unit_grad = (
        scale_value
        / (2.0 * batch_total)
        * jnp.dot(pair_weight, gathered, preferred_element_type=jnp.float32)
    )
    embed_grad = (
        unit_grad - unit_rows * jnp.sum(unit_rows * unit_grad, axis=-1, keepdims=True)
    ) / lengths
    return (loss_value, embed_grad[None])


def solution(mesh):
    in_specs = (P("dp", None), P("dp", None), P(), P(), P(), P(), P(), P("mod", "dp"))
    out_specs = (P(), P("mod", "dp", None))
    order = closed_path(mesh)

    def local(*args):
        batch_total = args[0].shape[0] * lax.axis_size("dp")
        if 4 * batch_total * batch_total <= SCORE_BYTES:
            return gather_both(order, *args)
        return gather_one(*args)

    return jax.shard_map(local, mesh=mesh, in_specs=in_specs, out_specs=out_specs, check_vma=False)
```

```python
import jax
import jax.numpy as jnp
import numpy as np
from jax import lax
from jax.experimental import pallas as pl
from jax.experimental.pallas import tpu as pltpu
from jax.sharding import PartitionSpec as P

LANES = 128
SIDE_INVERSE, SIDE_PLACE, SIDE_SCALE = 0, 1, 2
LOG2_E = float(np.log2(np.e))
SCORE_BYTES = 2**22
KERNEL_BYTES = 2**24


def closed_path(mesh):
    places = [getattr(d, "coords", None) for d in mesh.devices[0]]
    natural = list(range(len(places)))
    if any(p is None for p in places):
        return natural
    chips = {}
    for i, p in enumerate(places):
        chips.setdefault(tuple(p), []).append(i)
    span = [sorted({c[k] for c in chips}) for k in range(3)]
    wide = [k for k in range(3) if len(span[k]) > 1]
    if len(wide) != 2 or len(chips) != len(span[wide[0]]) * len(span[wide[1]]):
        return natural
    short, long = sorted(wide, key=lambda k: len(span[k]))
    if len(span[short]) != 2:
        return natural
    by = {(c[short], c[long]): v for c, v in chips.items()}
    there = [by[span[short][0], z] for z in span[long]]
    back = [by[span[short][1], z] for z in reversed(span[long])]
    return [i for cores in there + back for i in cores]


def from_partner(x, axis, bit):
    return lax.ppermute(x, axis, [(i, i ^ 1 << bit) for i in range(lax.axis_size(axis))])


def normalize_project(pooled, gain, weight):
    features = pooled.astype(jnp.float32)
    centered = features - jnp.mean(features, axis=-1, keepdims=True)
    variance = jnp.mean(centered * centered, axis=-1, keepdims=True)
    normalized = (centered * lax.rsqrt(variance + 1e-05) * gain).astype(jnp.bfloat16)
    return jnp.dot(normalized, weight, preferred_element_type=jnp.float32)


def unitize(embedded):
    lengths = jnp.sqrt(jnp.sum(embedded * embedded, axis=-1, keepdims=True) + 1e-06)
    return (embedded / lengths, lengths)


def similarity(left_rows, right_rows, scale_value):
    return scale_value * lax.dot_general(
        left_rows, right_rows, (((1,), (1,)), ((), ())), preferred_element_type=jnp.float32
    )


def log_sum_exp(scores, axis):
    top = jnp.max(scores, axis=axis)
    return top + jnp.log(jnp.sum(jnp.exp(scores - jnp.expand_dims(top, axis)), axis=axis))


def normalize(pooled, gain):
    features = pooled.astype(jnp.float32)
    centered = features - jnp.mean(features, axis=-1, keepdims=True)
    variance = jnp.mean(centered * centered, axis=-1, keepdims=True)
    return (centered * lax.rsqrt(variance + 1e-05) * gain).astype(jnp.bfloat16)


def lane_table(entries, shape):
    lane = lax.broadcasted_iota(jnp.int32, shape, 1)
    table = jnp.zeros(shape, jnp.float32)
    for i, entry in entries.items():
        table = jnp.where(lane == i, entry, table)
    return table


def embed_kernel(
    order,
    image_pooled,
    text_pooled,
    image_gain,
    text_gain,
    image_proj,
    text_proj,
    logit_scale,
    pair_index,
    sent,
    unit,
    side,
    image_rows,
    text_rows,
    image_scale,
    text_scale,
    image_weight,
    text_weight,
    scale_word,
    pair_row,
    arrived,
):
    row_count, width = unit.shape
    moves = [
        (pair_index, pair_row),
        (logit_scale, scale_word),
        (image_pooled, image_rows),
        (image_gain, image_scale),
        (text_pooled, text_rows),
        (text_gain, text_scale),
    ]
    copies = [pltpu.make_async_copy(a, b, arrived.at[i]) for i, (a, b) in enumerate(moves)]
    slabs = []
    for source, target in ((image_proj, image_weight), (text_proj, text_weight)):
        depth = 256 if source.shape[0] % 256 == 0 else source.shape[0]
        for start in range(0, source.shape[0], depth):
            rows = pl.ds(start, depth)
            copy = pltpu.make_async_copy(
                source.at[rows], target.at[rows], arrived.at[len(moves) + len(slabs)]
            )
            slabs.append((target, start, depth, copy))
    for copy in copies + [slab[3] for slab in slabs]:
        copy.start()

    copies[0].wait()
    copies[1].wait()
    pairs = pair_row[...]
    places = pairs
    for here, sample in enumerate(order):
        inside = (pairs >= sample * row_count) & (pairs < (sample + 1) * row_count)
        places = jnp.where(inside, pairs + (here - sample) * row_count, places)
    square = (row_count, row_count)
    upright = lax.broadcasted_iota(jnp.int32, square, 0) == lax.broadcasted_iota(jnp.int32, square, 1)
    place = jnp.sum(jnp.where(upright, places.astype(jnp.float32), 0.0), axis=1, keepdims=True)
    high = jnp.floor(place * (1.0 / LANES))
    digits = lane_table({0: high, 1: place - high * LANES}, (row_count, LANES))
    sent[:, 2 * width :] = digits.astype(jnp.bfloat16)

    copies[2].wait()
    copies[3].wait()
    image_normed = normalize(image_rows[...], image_scale[...][None, :])
    copies[4].wait()
    copies[5].wait()
    text_normed = normalize(text_rows[...], text_scale[...][None, :])

    def project(normed, weight):
        total = None
        for target, start, depth, copy in slabs:
            if target is weight:
                copy.wait()
                part = jnp.dot(
                    normed[:, start : start + depth],
                    target[start : start + depth, :],
                    preferred_element_type=jnp.float32,
                )
                total = part if total is None else total + part
        return total

    def unitize_rows(embedded):
        squares = jnp.sum(embedded * embedded, axis=-1, keepdims=True) + 1e-06
        inverse = 1.0 / jnp.sqrt(squares)
        return embedded * inverse, inverse

    is_image = lax.axis_index("mod") == 0
    image_unit, image_inverse = unitize_rows(project(image_normed, image_weight))
    text_unit, text_inverse = unitize_rows(project(text_normed, text_weight))
    own = jnp.where(is_image, image_unit, text_unit)
    unit[...] = own
    sent[:, :width] = own.astype(jnp.bfloat16)
    sent[:, width : 2 * width] = jnp.where(is_image, text_unit, image_unit).astype(jnp.bfloat16)
    side[...] = lane_table(
        {
            SIDE_INVERSE: jnp.where(is_image, image_inverse, text_inverse),
            SIDE_PLACE: place,
            SIDE_SCALE: scale_word[...][None, :],
        },
        (row_count, LANES),
    )


def score_kernel(order, every, unit, side, loss_value, embed_grad, scores):
    row_count, width = unit.shape
    batch_total = every.shape[0]
    chunk = LANES
    scale_value = side[0:1, SIDE_SCALE : SIDE_SCALE + 1]
    factor = scale_value * LOG2_E
    column = lax.broadcasted_iota(jnp.int32, (1, batch_total), 1).astype(jnp.float32)

    top = jnp.full((1, batch_total), -jnp.inf, jnp.float32)
    diagonal = jnp.zeros((1, batch_total), jnp.float32)
    rows_total = jnp.zeros((chunk, 1), jnp.float32)
    for start in range(0, batch_total, chunk):
        block = factor * lax.dot_general(
            every[start : start + chunk, :width],
            every[:, width : 2 * width],
            (((1,), (1,)), ((), ())),
            preferred_element_type=jnp.float32,
        )
        scores[start : start + chunk, :] = block
        top = jnp.maximum(top, jnp.max(block, axis=0, keepdims=True))
        digits = every[start : start + chunk, 2 * width :].astype(jnp.float32)
        places = digits[:, 0:1] * LANES + digits[:, 1:2]
        diagonal = diagonal + jnp.sum(jnp.where(column == places, block, 0.0), axis=0, keepdims=True)
        row_top = jnp.max(block, axis=1, keepdims=True)
        row_sum = jnp.sum(jnp.exp2(block - row_top), axis=1, keepdims=True)
        rows_total = rows_total + (row_top + LOG2_E * jnp.log(row_sum))
    column_sum = jnp.zeros((1, batch_total), jnp.float32)
    for start in range(0, batch_total, chunk):
        block = scores[start : start + chunk, :]
        column_sum = column_sum + jnp.sum(jnp.exp2(block - top), axis=0, keepdims=True)
    column_lse = top + LOG2_E * jnp.log(column_sum)
    total = jnp.sum(rows_total) + jnp.sum(column_lse - 2.0 * diagonal)
    loss_value[0] = total * (float(np.log(2.0)) / (2.0 * batch_total))

    mine = lax.axis_index("dp")
    first = jnp.int32(0)
    for here, sample in enumerate(order):
        first = jnp.where(mine == sample, here * row_count, first)
    block = scores[pl.ds(pl.multiple_of(first, 8), row_count), :]
    row_top = jnp.max(block, axis=1, keepdims=True)
    row_sum = jnp.sum(jnp.exp2(block - row_top), axis=1, keepdims=True)
    row_lse = row_top + LOG2_E * jnp.log(row_sum)
    matched = jnp.where(column == side[:, SIDE_PLACE : SIDE_PLACE + 1], 2.0, 0.0)
    pair_weight = jnp.exp2(block - row_lse) + jnp.exp2(block - column_lse) - matched
    unit_grad = (scale_value * (0.5 / batch_total)) * jnp.dot(
        pair_weight.astype(jnp.bfloat16),
        every[:, width : 2 * width],
        preferred_element_type=jnp.float32,
    )
    unit_rows = unit[...]
    along = jnp.sum(unit_rows * unit_grad, axis=-1, keepdims=True)
    embed_grad[0] = (unit_grad - unit_rows * along) * side[:, SIDE_INVERSE : SIDE_INVERSE + 1]


def gather_both(
    order, image_pooled, text_pooled, image_gain, text_gain, image_proj, text_proj, logit_scale, pair_index
):
    row_count = image_pooled.shape[0]
    width = image_proj.shape[1]
    batch_total = row_count * len(order)
    f32, bf16 = jnp.float32, jnp.bfloat16
    operands = (
        image_pooled, text_pooled, image_gain, text_gain, image_proj, text_proj, logit_scale, pair_index
    )
    sent, unit, side = pl.pallas_call(
        lambda *refs: embed_kernel(order, *refs),
        out_shape=(
            jax.ShapeDtypeStruct((row_count, 2 * width + LANES), bf16),
            jax.ShapeDtypeStruct((row_count, width), f32),
            jax.ShapeDtypeStruct((row_count, LANES), f32),
        ),
        in_specs=[pl.BlockSpec(memory_space=pltpu.HBM)] * len(operands),
        out_specs=[pl.BlockSpec(memory_space=pltpu.VMEM)] * 3,
        scratch_shapes=[pltpu.VMEM(x.shape, x.dtype) for x in operands]
        + [pltpu.SemaphoreType.DMA((64,))],
        compiler_params=pltpu.CompilerParams(vmem_limit_bytes=KERNEL_BYTES),
        name="embed",
    )(*(x if x.shape == (1,) else pltpu.with_memory_space_constraint(x, pltpu.HBM) for x in operands))
    every = lax.all_gather(
        sent.astype(jnp.float16), "dp", axis=0, tiled=True, axis_index_groups=[order]
    ).astype(bf16)
    loss_value, embed_grad = pl.pallas_call(
        lambda *refs: score_kernel(order, *refs),
        out_shape=(
            jax.ShapeDtypeStruct((1,), f32),
            jax.ShapeDtypeStruct((1, row_count, width), f32),
        ),
        in_specs=[pl.BlockSpec(memory_space=pltpu.VMEM)] * 3,
        out_specs=[pl.BlockSpec(memory_space=pltpu.SMEM), pl.BlockSpec(memory_space=pltpu.VMEM)],
        scratch_shapes=[pltpu.VMEM((batch_total, batch_total), f32)],
        compiler_params=pltpu.CompilerParams(vmem_limit_bytes=KERNEL_BYTES),
        name="scores",
    )(every, unit, side)
    return (loss_value[0], embed_grad)


def gather_one(
    image_pooled, text_pooled, image_gain, text_gain, image_proj, text_proj, logit_scale, pair_index
):
    module_index = lax.axis_index("mod")
    embedded = lax.cond(
        module_index == 0,
        lambda: normalize_project(image_pooled, image_gain, image_proj),
        lambda: normalize_project(text_pooled, text_gain, text_proj),
    )
    unit_rows, lengths = unitize(embedded)
    unit_half = unit_rows.astype(jnp.bfloat16)
    mirror_rows = from_partner(unit_half, "mod", 0)
    scale_value = logit_scale[0]
    row_count = unit_rows.shape[0]
    batch_total = row_count * lax.axis_size("dp")
    gathered = lax.all_gather(mirror_rows, "dp", axis=0, tiled=True)
    scores = similarity(unit_half, gathered, scale_value)
    own_lse = log_sum_exp(scores, 1)
    columns = lax.broadcasted_iota(jnp.int32, (row_count, batch_total), 1)
    matched = columns == pair_index[0][:, None]
    diagonal = jnp.sum(jnp.where(matched, scores, 0.0), axis=1)
    every_lse, every_diag = (
        lax.all_gather(own_lse, ("mod", "dp"), axis=0, tiled=True),
        lax.all_gather(diagonal, ("mod", "dp"), axis=0, tiled=True),
    )
    other_lse = lax.dynamic_slice_in_dim(every_lse, (1 - module_index) * batch_total, batch_total)
    loss_value = (jnp.sum(every_lse) - jnp.sum(every_diag)) / (2.0 * batch_total)
    pair_weight = (
        jnp.exp(scores - own_lse[:, None])
        + jnp.exp(scores - other_lse[None, :])
        - 2.0 * matched.astype(jnp.float32)
    ).astype(jnp.bfloat16)
    unit_grad = (
        scale_value
        / (2.0 * batch_total)
        * jnp.dot(pair_weight, gathered, preferred_element_type=jnp.float32)
    )
    embed_grad = (
        unit_grad - unit_rows * jnp.sum(unit_rows * unit_grad, axis=-1, keepdims=True)
    ) / lengths
    return (loss_value, embed_grad[None])


def solution(mesh):
    in_specs = (P("dp", None), P("dp", None), P(), P(), P(), P(), P(), P("mod", "dp"))
    out_specs = (P(), P("mod", "dp", None))
    order = closed_path(mesh)

    def local(*args):
        batch_total = args[0].shape[0] * lax.axis_size("dp")
        small = 4 * batch_total * batch_total <= SCORE_BYTES
        if small and batch_total % LANES == 0 and args[0].shape[0] % 8 == 0:
            return gather_both(order, *args)
        return gather_one(*args)

    return jax.shard_map(local, mesh=mesh, in_specs=in_specs, out_specs=out_specs, check_vma=False)
```

```python
import jax
import jax.numpy as jnp
import numpy as np
from jax import lax
from jax.experimental import pallas as pl
from jax.experimental.pallas import tpu as pltpu
from jax.sharding import PartitionSpec as P

LANES = 128
SIDE_INVERSE, SIDE_PLACE, SIDE_SCALE = 0, 1, 2
LOW_LANE = 64
LOG2_E = float(np.log2(np.e))
CHUNK = 256
SCORE_BYTES = 2**22
KERNEL_BYTES = 2**24


def closed_path(mesh):
    places = [getattr(d, "coords", None) for d in mesh.devices[0]]
    natural = list(range(len(places)))
    if any(p is None for p in places):
        return natural
    chips = {}
    for i, p in enumerate(places):
        chips.setdefault(tuple(p), []).append(i)
    span = [sorted({c[k] for c in chips}) for k in range(3)]
    wide = [k for k in range(3) if len(span[k]) > 1]
    if len(wide) != 2 or len(chips) != len(span[wide[0]]) * len(span[wide[1]]):
        return natural
    short, long = sorted(wide, key=lambda k: len(span[k]))
    if len(span[short]) != 2:
        return natural
    by = {(c[short], c[long]): v for c, v in chips.items()}
    there = [by[span[short][0], z] for z in span[long]]
    back = [by[span[short][1], z] for z in reversed(span[long])]
    return [i for cores in there + back for i in cores]


def from_partner(x, axis, bit):
    return lax.ppermute(x, axis, [(i, i ^ 1 << bit) for i in range(lax.axis_size(axis))])


def normalize_project(pooled, gain, weight):
    features = pooled.astype(jnp.float32)
    centered = features - jnp.mean(features, axis=-1, keepdims=True)
    variance = jnp.mean(centered * centered, axis=-1, keepdims=True)
    normalized = (centered * lax.rsqrt(variance + 1e-05) * gain).astype(jnp.bfloat16)
    return jnp.dot(normalized, weight, preferred_element_type=jnp.float32)


def unitize(embedded):
    lengths = jnp.sqrt(jnp.sum(embedded * embedded, axis=-1, keepdims=True) + 1e-06)
    return (embedded / lengths, lengths)


def similarity(left_rows, right_rows, scale_value):
    return scale_value * lax.dot_general(
        left_rows, right_rows, (((1,), (1,)), ((), ())), preferred_element_type=jnp.float32
    )


def log_sum_exp(scores, axis):
    top = jnp.max(scores, axis=axis)
    return top + jnp.log(jnp.sum(jnp.exp(scores - jnp.expand_dims(top, axis)), axis=axis))


def normalize(pooled, gain):
    features = pooled.astype(jnp.float32)
    centered = features - jnp.mean(features, axis=-1, keepdims=True)
    variance = jnp.mean(centered * centered, axis=-1, keepdims=True)
    return (centered * lax.rsqrt(variance + 1e-05) * gain).astype(jnp.bfloat16)


def lane_table(entries, shape):
    lane = lax.broadcasted_iota(jnp.int32, shape, 1)
    table = jnp.zeros(shape, jnp.float32)
    for i, entry in entries.items():
        table = jnp.where(lane == i, entry, table)
    return table


def embed_kernel(
    order,
    image_pooled,
    text_pooled,
    image_gain,
    text_gain,
    image_proj,
    text_proj,
    pair_index,
    sent,
    unit,
    side,
    image_rows,
    text_rows,
    image_scale,
    text_scale,
    image_weight,
    text_weight,
    pair_row,
    arrived,
):
    row_count, width = unit.shape
    moves = [
        (pair_index, pair_row),
        (image_pooled, image_rows),
        (image_gain, image_scale),
        (text_pooled, text_rows),
        (text_gain, text_scale),
        (image_proj, image_weight),
        (text_proj, text_weight),
    ]
    copies = [pltpu.make_async_copy(a, b, arrived.at[i]) for i, (a, b) in enumerate(moves)]
    for copy in copies:
        copy.start()

    copies[0].wait()
    pairs = pair_row[...]
    places = pairs
    for here, sample in enumerate(order):
        inside = (pairs >= sample * row_count) & (pairs < (sample + 1) * row_count)
        places = jnp.where(inside, pairs + (here - sample) * row_count, places)
    square = (row_count, row_count)
    upright = lax.broadcasted_iota(jnp.int32, square, 0) == lax.broadcasted_iota(jnp.int32, square, 1)
    place = jnp.sum(jnp.where(upright, places.astype(jnp.float32), 0.0), axis=1, keepdims=True)
    high = jnp.floor(place * (1.0 / LANES))
    across, down = width // LANES, row_count // 8
    for k in range(down):
        rows = slice(k * 8, k * 8 + 8)
        lane = lax.broadcasted_iota(jnp.int32, (8, LANES), 1)
        tile = jnp.where(lane == k, high[rows], 0.0 if k == 0 else tile)
        tile = jnp.where(lane == LOW_LANE + k, place[rows] - high[rows] * LANES, tile)
    sent[2 * across * down] = tile.astype(jnp.bfloat16)

    copies[1].wait()
    copies[2].wait()
    image_normed = normalize(image_rows[...], image_scale[...][None, :])
    copies[3].wait()
    copies[4].wait()
    text_normed = normalize(text_rows[...], text_scale[...][None, :])

    def project(normed, weight):
        return jnp.dot(normed, weight, preferred_element_type=jnp.float32)

    def unitize_rows(embedded):
        squares = jnp.sum(embedded * embedded, axis=-1, keepdims=True) + 1e-06
        inverse = 1.0 / jnp.sqrt(squares)
        return embedded * inverse, inverse

    is_image = lax.axis_index("mod") == 0
    copies[5].wait()
    image_unit, image_inverse = unitize_rows(project(image_normed, image_weight[...]))
    copies[6].wait()
    text_unit, text_inverse = unitize_rows(project(text_normed, text_weight[...]))
    own = jnp.where(is_image, image_unit, text_unit)
    unit[...] = own
    other = jnp.where(is_image, text_unit, image_unit)
    for base, rows in ((0, own), (across * down, other)):
        for i in range(down):
            for k in range(across):
                tile = rows[i * 8 : i * 8 + 8, k * LANES : (k + 1) * LANES]
                sent[base + i * across + k] = tile.astype(jnp.bfloat16)
    side[...] = lane_table(
        {
            SIDE_INVERSE: jnp.where(is_image, image_inverse, text_inverse),
            SIDE_PLACE: place,
        },
        (row_count, LANES),
    )


def score_kernel(order, logit_scale, own_all, other_all, digits, unit, side, loss_value, embed_grad, scores):
    row_count, width = unit.shape
    batch_total = own_all.shape[0]
    scale_value = logit_scale[0]
    factor = scale_value * LOG2_E
    column = lax.broadcasted_iota(jnp.int32, (1, batch_total), 1).astype(jnp.float32)

    columns = digits[...].astype(jnp.float32)
    columns = columns * LANES + pltpu.roll(columns, LANES - LOW_LANE, axis=2)
    places = jnp.concatenate(
        [columns[i, :, k : k + 1] for i in range(len(order)) for k in range(row_count // 8)], axis=0
    )
    lanes = lax.broadcasted_iota(jnp.int32, (1, LANES), 1).astype(jnp.float32)
    row_tops = jnp.full((batch_total, LANES), -jnp.inf, jnp.float32)
    diagonal = jnp.zeros((8, LANES), jnp.float32)
    column_lses = []
    for start in range(0, batch_total, CHUNK):
        count = min(CHUNK, batch_total - start)
        block = factor * lax.dot_general(
            own_all[...],
            other_all[start : start + count, :],
            (((1,), (1,)), ((), ())),
            preferred_element_type=jnp.float32,
        )
        scores[:, start : start + count] = block
        top = jnp.max(block, axis=0, keepdims=True)
        total = jnp.sum(jnp.exp2(block - top), axis=0, keepdims=True)
        column_lses.append(top + LOG2_E * jnp.log(total))
        for k in range(0, count, LANES):
            part = block[:, k : k + LANES]
            row_tops = jnp.maximum(row_tops, part)
            hit = jnp.where(places == lanes + (start + k), part, 0.0)
            diagonal = diagonal + jnp.sum(hit.reshape(batch_total // 8, 8, LANES), axis=0)
    column_lse = jnp.concatenate(column_lses, axis=1)
    row_top = jnp.max(row_tops, axis=1, keepdims=True)
    sums = jnp.zeros((batch_total, LANES), jnp.float32)
    for start in range(0, batch_total, LANES):
        sums = sums + jnp.exp2(scores[:, start : start + LANES] - row_top)
    row_lse = row_top + LOG2_E * jnp.log(jnp.sum(sums, axis=1, keepdims=True))
    total = jnp.sum(row_lse) + jnp.sum(column_lse) - 2.0 * jnp.sum(diagonal)
    loss_value[0] = total * (float(np.log(2.0)) / (2.0 * batch_total))

    mine = lax.axis_index("dp")
    first = jnp.int32(0)
    for here, sample in enumerate(order):
        first = jnp.where(mine == sample, here * row_count, first)
    block = scores[pl.ds(pl.multiple_of(first, 8), row_count), :]
    row_top = jnp.max(block, axis=1, keepdims=True)
    row_sum = jnp.sum(jnp.exp2(block - row_top), axis=1, keepdims=True)
    row_lse = row_top + LOG2_E * jnp.log(row_sum)
    matched = jnp.where(column == side[:, SIDE_PLACE : SIDE_PLACE + 1], 2.0, 0.0)
    pair_weight = jnp.exp2(block - row_lse) + jnp.exp2(block - column_lse) - matched
    unit_grad = (scale_value * (0.5 / batch_total)) * jnp.dot(
        pair_weight.astype(jnp.bfloat16),
        other_all[...],
        preferred_element_type=jnp.float32,
    )
    unit_rows = unit[...]
    along = jnp.sum(unit_rows * unit_grad, axis=-1, keepdims=True)
    embed_grad[0] = (unit_grad - unit_rows * along) * side[:, SIDE_INVERSE : SIDE_INVERSE + 1]


def gather_both(
    order, image_pooled, text_pooled, image_gain, text_gain, image_proj, text_proj, logit_scale, pair_index
):
    row_count = image_pooled.shape[0]
    width = image_proj.shape[1]
    batch_total = row_count * len(order)
    f32, bf16 = jnp.float32, jnp.bfloat16
    tiles = row_count * width // (8 * LANES)
    operands = (
        image_pooled, text_pooled, image_gain, text_gain, image_proj, text_proj, pair_index
    )
    sent, unit, side = pl.pallas_call(
        lambda *refs: embed_kernel(order, *refs),
        out_shape=(
            jax.ShapeDtypeStruct((2 * tiles + 1, 8, LANES), bf16),
            jax.ShapeDtypeStruct((row_count, width), f32),
            jax.ShapeDtypeStruct((row_count, LANES), f32),
        ),
        in_specs=[pl.BlockSpec(memory_space=pltpu.HBM)] * len(operands),
        out_specs=[pl.BlockSpec(memory_space=pltpu.VMEM)] * 3,
        scratch_shapes=[pltpu.VMEM(x.shape, x.dtype) for x in operands]
        + [pltpu.SemaphoreType.DMA((len(operands),))],
        compiler_params=pltpu.CompilerParams(vmem_limit_bytes=KERNEL_BYTES),
        name="embed",
    )(*(pltpu.with_memory_space_constraint(x, pltpu.HBM) for x in operands))
    every = lax.all_gather(
        sent.astype(jnp.float16), "dp", axis=0, tiled=True, axis_index_groups=[order]
    ).reshape(len(order), 2 * tiles + 1, 8, LANES)

    def plain(blocks):
        blocks = blocks.reshape(len(order), row_count // 8, width // LANES, 8, LANES)
        return blocks.transpose(0, 1, 3, 2, 4).reshape(batch_total, width).astype(bf16)

    own_all = plain(every[:, :tiles])
    other_all = plain(every[:, tiles : 2 * tiles])
    digits = every[:, 2 * tiles].astype(bf16)
    loss_value, embed_grad = pl.pallas_call(
        lambda *refs: score_kernel(order, *refs),
        out_shape=(
            jax.ShapeDtypeStruct((1,), f32),
            jax.ShapeDtypeStruct((1, row_count, width), f32),
        ),
        in_specs=[pl.BlockSpec(memory_space=pltpu.SMEM)] + [pl.BlockSpec(memory_space=pltpu.VMEM)] * 5,
        out_specs=[pl.BlockSpec(memory_space=pltpu.SMEM), pl.BlockSpec(memory_space=pltpu.VMEM)],
        scratch_shapes=[pltpu.VMEM((batch_total, batch_total), f32)],
        compiler_params=pltpu.CompilerParams(vmem_limit_bytes=KERNEL_BYTES),
        name="scores",
    )(logit_scale, own_all, other_all, digits, unit, side)
    return (loss_value[0], embed_grad)


def gather_one(
    image_pooled, text_pooled, image_gain, text_gain, image_proj, text_proj, logit_scale, pair_index
):
    module_index = lax.axis_index("mod")
    embedded = lax.cond(
        module_index == 0,
        lambda: normalize_project(image_pooled, image_gain, image_proj),
        lambda: normalize_project(text_pooled, text_gain, text_proj),
    )
    unit_rows, lengths = unitize(embedded)
    unit_half = unit_rows.astype(jnp.bfloat16)
    mirror_rows = from_partner(unit_half, "mod", 0)
    scale_value = logit_scale[0]
    row_count = unit_rows.shape[0]
    batch_total = row_count * lax.axis_size("dp")
    gathered = lax.all_gather(mirror_rows, "dp", axis=0, tiled=True)
    scores = similarity(unit_half, gathered, scale_value)
    own_lse = log_sum_exp(scores, 1)
    columns = lax.broadcasted_iota(jnp.int32, (row_count, batch_total), 1)
    matched = columns == pair_index[0][:, None]
    diagonal = jnp.sum(jnp.where(matched, scores, 0.0), axis=1)
    every_lse, every_diag = (
        lax.all_gather(own_lse, ("mod", "dp"), axis=0, tiled=True),
        lax.all_gather(diagonal, ("mod", "dp"), axis=0, tiled=True),
    )
    other_lse = lax.dynamic_slice_in_dim(every_lse, (1 - module_index) * batch_total, batch_total)
    loss_value = (jnp.sum(every_lse) - jnp.sum(every_diag)) / (2.0 * batch_total)
    pair_weight = (
        jnp.exp(scores - own_lse[:, None])
        + jnp.exp(scores - other_lse[None, :])
        - 2.0 * matched.astype(jnp.float32)
    ).astype(jnp.bfloat16)
    unit_grad = (
        scale_value
        / (2.0 * batch_total)
        * jnp.dot(pair_weight, gathered, preferred_element_type=jnp.float32)
    )
    embed_grad = (
        unit_grad - unit_rows * jnp.sum(unit_rows * unit_grad, axis=-1, keepdims=True)
    ) / lengths
    return (loss_value, embed_grad[None])


def solution(mesh):
    in_specs = (P("dp", None), P("dp", None), P(), P(), P(), P(), P(), P("mod", "dp"))
    out_specs = (P(), P("mod", "dp", None))
    order = closed_path(mesh)

    def local(*args):
        batch_total = args[0].shape[0] * lax.axis_size("dp")
        small = 4 * batch_total * batch_total <= SCORE_BYTES
        width = args[4].shape[1]
        if small and batch_total % LANES == 0 and args[0].shape[0] % 8 == 0 and width % LANES == 0:
            return gather_both(order, *args)
        return gather_one(*args)

    return jax.shard_map(local, mesh=mesh, in_specs=in_specs, out_specs=out_specs, check_vma=False)
```

```python
import jax
import jax.numpy as jnp
import numpy as np
from jax import lax
from jax.experimental import pallas as pl
from jax.experimental.pallas import tpu as pltpu
from jax.sharding import PartitionSpec as P

LANES = 128
SIDE_INVERSE, SIDE_PLACE, SIDE_SCALE = 0, 1, 2
LOW_LANE = 64
LOG2_E = float(np.log2(np.e))
CHUNK = 256
SCORE_BYTES = 2**22
KERNEL_BYTES = 2**24
NORM_COST = 925_000_000


def closed_path(mesh):
    places = [getattr(d, "coords", None) for d in mesh.devices[0]]
    natural = list(range(len(places)))
    if any(p is None for p in places):
        return natural
    chips = {}
    for i, p in enumerate(places):
        chips.setdefault(tuple(p), []).append(i)
    span = [sorted({c[k] for c in chips}) for k in range(3)]
    wide = [k for k in range(3) if len(span[k]) > 1]
    if len(wide) != 2 or len(chips) != len(span[wide[0]]) * len(span[wide[1]]):
        return natural
    short, long = sorted(wide, key=lambda k: len(span[k]))
    if len(span[short]) != 2:
        return natural
    by = {(c[short], c[long]): v for c, v in chips.items()}
    there = [by[span[short][0], z] for z in span[long]]
    back = [by[span[short][1], z] for z in reversed(span[long])]
    return [i for cores in there + back for i in cores]


def from_partner(x, axis, bit):
    return lax.ppermute(x, axis, [(i, i ^ 1 << bit) for i in range(lax.axis_size(axis))])


def normalize_project(pooled, gain, weight):
    features = pooled.astype(jnp.float32)
    centered = features - jnp.mean(features, axis=-1, keepdims=True)
    variance = jnp.mean(centered * centered, axis=-1, keepdims=True)
    normalized = (centered * lax.rsqrt(variance + 1e-05) * gain).astype(jnp.bfloat16)
    return jnp.dot(normalized, weight, preferred_element_type=jnp.float32)


def unitize(embedded):
    lengths = jnp.sqrt(jnp.sum(embedded * embedded, axis=-1, keepdims=True) + 1e-06)
    return (embedded / lengths, lengths)


def similarity(left_rows, right_rows, scale_value):
    return scale_value * lax.dot_general(
        left_rows, right_rows, (((1,), (1,)), ((), ())), preferred_element_type=jnp.float32
    )


def log_sum_exp(scores, axis):
    top = jnp.max(scores, axis=axis)
    return top + jnp.log(jnp.sum(jnp.exp(scores - jnp.expand_dims(top, axis)), axis=axis))


def normalize(pooled, gain):
    features = pooled.astype(jnp.float32)
    centered = features - jnp.mean(features, axis=-1, keepdims=True)
    variance = jnp.mean(centered * centered, axis=-1, keepdims=True)
    return (centered * lax.rsqrt(variance + 1e-05) * gain).astype(jnp.bfloat16)


def lane_table(entries, shape):
    lane = lax.broadcasted_iota(jnp.int32, shape, 1)
    table = jnp.zeros(shape, jnp.float32)
    for i, entry in entries.items():
        table = jnp.where(lane == i, entry, table)
    return table


def norm_kernel(
    order,
    image_pooled,
    text_pooled,
    image_gain,
    text_gain,
    pair_index,
    image_normed,
    text_normed,
    side,
):
    row_count = image_pooled.shape[0]
    pairs = pair_index[...]
    places = pairs
    for here, sample in enumerate(order):
        inside = (pairs >= sample * row_count) & (pairs < (sample + 1) * row_count)
        places = jnp.where(inside, pairs + (here - sample) * row_count, places)
    square = (row_count, row_count)
    upright = lax.broadcasted_iota(jnp.int32, square, 0) == lax.broadcasted_iota(jnp.int32, square, 1)
    place = jnp.sum(jnp.where(upright, places.astype(jnp.float32), 0.0), axis=1, keepdims=True)
    side[...] = jnp.broadcast_to(place, side.shape)
    image_normed[...] = normalize(image_pooled[...], image_gain[...][None, :])
    text_normed[...] = normalize(text_pooled[...], text_gain[...][None, :])


def embed_kernel(
    logit_scale, image_normed, text_normed, image_weight, text_weight, spots, sent, unit, side
):
    row_count, width = unit.shape
    place = spots[:, 0:1]
    high = jnp.floor(place * (1.0 / LANES))
    across, down = width // LANES, row_count // 8
    for k in range(down):
        rows = slice(k * 8, k * 8 + 8)
        lane = lax.broadcasted_iota(jnp.int32, (8, LANES), 1)
        tile = jnp.where(lane == k, high[rows], 0.0 if k == 0 else tile)
        tile = jnp.where(lane == LOW_LANE + k, place[rows] - high[rows] * LANES, tile)
    sent[2 * across * down] = tile.astype(jnp.bfloat16)

    def unitize_rows(normed, weight):
        embedded = jnp.dot(normed[...], weight[...], preferred_element_type=jnp.float32)
        squares = jnp.sum(embedded * embedded, axis=-1, keepdims=True) + 1e-06
        inverse = 1.0 / jnp.sqrt(squares)
        return embedded * inverse, inverse

    is_image = lax.axis_index("mod") == 0
    image_unit, image_inverse = unitize_rows(image_normed, image_weight)
    text_unit, text_inverse = unitize_rows(text_normed, text_weight)
    own = jnp.where(is_image, image_unit, text_unit)
    unit[...] = own
    other = jnp.where(is_image, text_unit, image_unit)
    for base, rows in ((0, own), (across * down, other)):
        for i in range(down):
            for k in range(across):
                tile = rows[i * 8 : i * 8 + 8, k * LANES : (k + 1) * LANES]
                sent[base + i * across + k] = tile.astype(jnp.bfloat16)
    side[...] = lane_table(
        {
            SIDE_INVERSE: jnp.where(is_image, image_inverse, text_inverse),
            SIDE_PLACE: place,
            SIDE_SCALE: logit_scale[0],
        },
        (row_count, LANES),
    )


def fold_rows(block, reduce):
    rows, lanes = block.shape
    if rows % 64 == 0:
        block = reduce(block.reshape(rows // 64, 64, lanes), axis=0)
    return reduce(block, axis=0, keepdims=True)


def score_kernel(order, own_all, other_all, digits, unit, side, loss_value, embed_grad, scores):
    row_count, width = unit.shape
    batch_total = own_all.shape[0]
    scale_value = side[0:1, SIDE_SCALE : SIDE_SCALE + 1]
    factor = scale_value * LOG2_E
    column = lax.broadcasted_iota(jnp.int32, (1, batch_total), 1).astype(jnp.float32)

    columns = digits[...].astype(jnp.float32)
    columns = columns * LANES + pltpu.roll(columns, LANES - LOW_LANE, axis=2)
    places = jnp.concatenate(
        [columns[i, :, k : k + 1] for i in range(len(order)) for k in range(row_count // 8)], axis=0
    )
    lanes = lax.broadcasted_iota(jnp.int32, (1, LANES), 1).astype(jnp.float32)
    row_tops = jnp.full((batch_total, LANES), -jnp.inf, jnp.float32)
    diagonal = jnp.zeros((batch_total, LANES), jnp.float32)
    column_lses = []
    for start in range(0, batch_total, CHUNK):
        count = min(CHUNK, batch_total - start)
        block = factor * lax.dot_general(
            own_all[...],
            other_all[start : start + count, :],
            (((1,), (1,)), ((), ())),
            preferred_element_type=jnp.float32,
        )
        scores[:, start : start + count] = block
        top = fold_rows(block, jnp.max)
        total = fold_rows(jnp.exp2(block - top), jnp.sum)
        column_lses.append(top + LOG2_E * jnp.log(total))
        for k in range(0, count, LANES):
            part = block[:, k : k + LANES]
            row_tops = jnp.maximum(row_tops, part)
            diagonal = jnp.where(places == lanes + (start + k), part, diagonal)
    column_lse = jnp.concatenate(column_lses, axis=1)
    mine = lax.axis_index("dp")
    first = jnp.int32(0)
    for here, sample in enumerate(order):
        first = jnp.where(mine == sample, here * row_count, first)
    block = scores[pl.ds(pl.multiple_of(first, 8), row_count), :]
    row_top = jnp.max(block, axis=1, keepdims=True)
    row_sum = jnp.sum(jnp.exp2(block - row_top), axis=1, keepdims=True)
    row_lse = row_top + LOG2_E * jnp.log(row_sum)
    matched = jnp.where(column == side[:, SIDE_PLACE : SIDE_PLACE + 1], 2.0, 0.0)
    pair_weight = jnp.exp2(block - row_lse) + jnp.exp2(block - column_lse) - matched
    unit_grad = (scale_value * (0.5 / batch_total)) * jnp.dot(
        pair_weight.astype(jnp.bfloat16),
        other_all[...],
        preferred_element_type=jnp.float32,
    )
    unit_rows = unit[...]
    along = jnp.sum(unit_rows * unit_grad, axis=-1, keepdims=True)
    embed_grad[0] = (unit_grad - unit_rows * along) * side[:, SIDE_INVERSE : SIDE_INVERSE + 1]

    row_top = jnp.max(row_tops, axis=1, keepdims=True)
    sums = jnp.zeros((batch_total, LANES), jnp.float32)
    for start in range(0, batch_total, LANES):
        sums = sums + jnp.exp2(scores[:, start : start + LANES] - row_top)
    row_lse = row_top + LOG2_E * jnp.log(jnp.sum(sums, axis=1, keepdims=True))
    total = jnp.sum(fold_rows(row_lse, jnp.sum)) + jnp.sum(column_lse) - 2.0 * jnp.sum(fold_rows(diagonal, jnp.sum))
    loss_value[0] = total * (float(np.log(2.0)) / (2.0 * batch_total))


def gather_both(
    order, image_pooled, text_pooled, image_gain, text_gain, image_proj, text_proj, logit_scale, pair_index
):
    row_count = image_pooled.shape[0]
    width = image_proj.shape[1]
    batch_total = row_count * len(order)
    f32, bf16 = jnp.float32, jnp.bfloat16
    tiles = row_count * width // (8 * LANES)
    operands = (image_pooled, text_pooled, image_gain, text_gain, pair_index)
    image_normed, text_normed, spots = pl.pallas_call(
        lambda *refs: norm_kernel(order, *refs),
        out_shape=(
            jax.ShapeDtypeStruct(image_pooled.shape, bf16),
            jax.ShapeDtypeStruct(text_pooled.shape, bf16),
            jax.ShapeDtypeStruct((row_count, LANES), f32),
        ),
        in_specs=[pl.BlockSpec(memory_space=pltpu.VMEM)] * len(operands),
        out_specs=[pl.BlockSpec(memory_space=pltpu.VMEM)] * 3,
        compiler_params=pltpu.CompilerParams(vmem_limit_bytes=KERNEL_BYTES),
        cost_estimate=pl.CostEstimate(flops=NORM_COST, bytes_accessed=4_000_000, transcendentals=0),
        name="norm",
    )(*(pltpu.with_memory_space_constraint(x, pltpu.HBM) for x in operands))
    sent, unit, side = pl.pallas_call(
        embed_kernel,
        out_shape=(
            jax.ShapeDtypeStruct((2 * tiles + 1, 8, LANES), bf16),
            jax.ShapeDtypeStruct((row_count, width), f32),
            jax.ShapeDtypeStruct((row_count, LANES), f32),
        ),
        in_specs=[pl.BlockSpec(memory_space=pltpu.SMEM)] + [pl.BlockSpec(memory_space=pltpu.VMEM)] * 5,
        out_specs=[pl.BlockSpec(memory_space=pltpu.VMEM)] * 3,
        compiler_params=pltpu.CompilerParams(vmem_limit_bytes=KERNEL_BYTES),
        name="embed",
    )(logit_scale, image_normed, text_normed, image_proj, text_proj, spots)
    every = lax.all_gather(
        sent.astype(jnp.float16), "dp", axis=0, tiled=True, axis_index_groups=[order]
    ).reshape(len(order), 2 * tiles + 1, 8, LANES)

    def plain(blocks):
        blocks = blocks.reshape(len(order), row_count // 8, width // LANES, 8, LANES)
        return blocks.transpose(0, 1, 3, 2, 4).reshape(batch_total, width).astype(bf16)

    own_all = plain(every[:, :tiles])
    other_all = plain(every[:, tiles : 2 * tiles])
    digits = every[:, 2 * tiles].astype(bf16)
    loss_value, embed_grad = pl.pallas_call(
        lambda *refs: score_kernel(order, *refs),
        out_shape=(
            jax.ShapeDtypeStruct((1,), f32),
            jax.ShapeDtypeStruct((1, row_count, width), f32),
        ),
        in_specs=[pl.BlockSpec(memory_space=pltpu.VMEM)] * 5,
        out_specs=[pl.BlockSpec(memory_space=pltpu.SMEM), pl.BlockSpec(memory_space=pltpu.VMEM)],
        scratch_shapes=[pltpu.VMEM((batch_total, batch_total), f32)],
        compiler_params=pltpu.CompilerParams(vmem_limit_bytes=KERNEL_BYTES),
        name="scores",
    )(own_all, other_all, digits, unit, side)
    return (loss_value[0], embed_grad)


def gather_one(
    image_pooled, text_pooled, image_gain, text_gain, image_proj, text_proj, logit_scale, pair_index
):
    module_index = lax.axis_index("mod")
    embedded = lax.cond(
        module_index == 0,
        lambda: normalize_project(image_pooled, image_gain, image_proj),
        lambda: normalize_project(text_pooled, text_gain, text_proj),
    )
    unit_rows, lengths = unitize(embedded)
    unit_half = unit_rows.astype(jnp.bfloat16)
    mirror_rows = from_partner(unit_half, "mod", 0)
    scale_value = logit_scale[0]
    row_count = unit_rows.shape[0]
    batch_total = row_count * lax.axis_size("dp")
    gathered = lax.all_gather(mirror_rows, "dp", axis=0, tiled=True)
    scores = similarity(unit_half, gathered, scale_value)
    own_lse = log_sum_exp(scores, 1)
    columns = lax.broadcasted_iota(jnp.int32, (row_count, batch_total), 1)
    matched = columns == pair_index[0][:, None]
    diagonal = jnp.sum(jnp.where(matched, scores, 0.0), axis=1)
    every_lse, every_diag = (
        lax.all_gather(own_lse, ("mod", "dp"), axis=0, tiled=True),
        lax.all_gather(diagonal, ("mod", "dp"), axis=0, tiled=True),
    )
    other_lse = lax.dynamic_slice_in_dim(every_lse, (1 - module_index) * batch_total, batch_total)
    loss_value = (jnp.sum(every_lse) - jnp.sum(every_diag)) / (2.0 * batch_total)
    pair_weight = (
        jnp.exp(scores - own_lse[:, None])
        + jnp.exp(scores - other_lse[None, :])
        - 2.0 * matched.astype(jnp.float32)
    ).astype(jnp.bfloat16)
    unit_grad = (
        scale_value
        / (2.0 * batch_total)
        * jnp.dot(pair_weight, gathered, preferred_element_type=jnp.float32)
    )
    embed_grad = (
        unit_grad - unit_rows * jnp.sum(unit_rows * unit_grad, axis=-1, keepdims=True)
    ) / lengths
    return (loss_value, embed_grad[None])


def solution(mesh):
    in_specs = (P("dp", None), P("dp", None), P(), P(), P(), P(), P(), P("mod", "dp"))
    out_specs = (P(), P("mod", "dp", None))
    order = closed_path(mesh)

    def local(*args):
        batch_total = args[0].shape[0] * lax.axis_size("dp")
        small = 4 * batch_total * batch_total <= SCORE_BYTES
        width = args[4].shape[1]
        if small and batch_total % LANES == 0 and args[0].shape[0] % 8 == 0 and width % LANES == 0:
            return gather_both(order, *args)
        return gather_one(*args)

    return jax.shard_map(local, mesh=mesh, in_specs=in_specs, out_specs=out_specs, check_vma=False)
```

```python
import jax
import jax.numpy as jnp
import numpy as np
from jax import lax
from jax.experimental import pallas as pl
from jax.experimental.pallas import tpu as pltpu
from jax.sharding import PartitionSpec as P

LANES = 128
SIDE_INVERSE, SIDE_PLACE, SIDE_SCALE = 0, 1, 2
LOW_LANE = 64
LOG2_E = float(np.log2(np.e))
CHUNK = 256
SCORE_BYTES = 2**22
KERNEL_BYTES = 2**24
NORM_COST = 100_000_000
SCALE_COST = 800_000_000


def closed_path(mesh):
    places = [getattr(d, "coords", None) for d in mesh.devices[0]]
    natural = list(range(len(places)))
    if any(p is None for p in places):
        return natural
    chips = {}
    for i, p in enumerate(places):
        chips.setdefault(tuple(p), []).append(i)
    span = [sorted({c[k] for c in chips}) for k in range(3)]
    wide = [k for k in range(3) if len(span[k]) > 1]
    if len(wide) != 2 or len(chips) != len(span[wide[0]]) * len(span[wide[1]]):
        return natural
    short, long = sorted(wide, key=lambda k: len(span[k]))
    if len(span[short]) != 2:
        return natural
    by = {(c[short], c[long]): v for c, v in chips.items()}
    there = [by[span[short][0], z] for z in span[long]]
    back = [by[span[short][1], z] for z in reversed(span[long])]
    return [i for cores in there + back for i in cores]


def from_partner(x, axis, bit):
    return lax.ppermute(x, axis, [(i, i ^ 1 << bit) for i in range(lax.axis_size(axis))])


def normalize_project(pooled, gain, weight):
    features = pooled.astype(jnp.float32)
    centered = features - jnp.mean(features, axis=-1, keepdims=True)
    variance = jnp.mean(centered * centered, axis=-1, keepdims=True)
    normalized = (centered * lax.rsqrt(variance + 1e-05) * gain).astype(jnp.bfloat16)
    return jnp.dot(normalized, weight, preferred_element_type=jnp.float32)


def unitize(embedded):
    lengths = jnp.sqrt(jnp.sum(embedded * embedded, axis=-1, keepdims=True) + 1e-06)
    return (embedded / lengths, lengths)


def similarity(left_rows, right_rows, scale_value):
    return scale_value * lax.dot_general(
        left_rows, right_rows, (((1,), (1,)), ((), ())), preferred_element_type=jnp.float32
    )


def log_sum_exp(scores, axis):
    top = jnp.max(scores, axis=axis)
    return top + jnp.log(jnp.sum(jnp.exp(scores - jnp.expand_dims(top, axis)), axis=axis))


def normalize(pooled, gain):
    features = pooled.astype(jnp.float32)
    centered = features - jnp.mean(features, axis=-1, keepdims=True)
    variance = jnp.mean(centered * centered, axis=-1, keepdims=True)
    return (centered * lax.rsqrt(variance + 1e-05) * gain).astype(jnp.bfloat16)


def lane_table(entries, shape):
    lane = lax.broadcasted_iota(jnp.int32, shape, 1)
    table = jnp.zeros(shape, jnp.float32)
    for i, entry in entries.items():
        table = jnp.where(lane == i, entry, table)
    return table


def scale_kernel(logit_scale, spread):
    spread[...] = jnp.full(spread.shape, logit_scale[0], jnp.float32)


def norm_kernel(
    order,
    spread,
    image_pooled,
    text_pooled,
    image_gain,
    text_gain,
    pair_index,
    image_normed,
    text_normed,
    side,
):
    row_count = image_pooled.shape[0]
    pairs = pair_index[...]
    places = pairs
    for here, sample in enumerate(order):
        inside = (pairs >= sample * row_count) & (pairs < (sample + 1) * row_count)
        places = jnp.where(inside, pairs + (here - sample) * row_count, places)
    square = (row_count, row_count)
    upright = lax.broadcasted_iota(jnp.int32, square, 0) == lax.broadcasted_iota(jnp.int32, square, 1)
    place = jnp.sum(jnp.where(upright, places.astype(jnp.float32), 0.0), axis=1, keepdims=True)
    shape = side.shape
    side[...] = lane_table({SIDE_PLACE: place, SIDE_SCALE: spread[0:1, 0:1]}, shape)
    image_normed[...] = normalize(image_pooled[...], image_gain[...][None, :])
    text_normed[...] = normalize(text_pooled[...], text_gain[...][None, :])


def embed_kernel(
    image_normed, text_normed, image_weight, text_weight, spots, sent, unit, side
):
    row_count, width = unit.shape
    place = spots[:, SIDE_PLACE : SIDE_PLACE + 1]
    high = jnp.floor(place * (1.0 / LANES))
    across, down = width // LANES, row_count // 8
    for k in range(down):
        rows = slice(k * 8, k * 8 + 8)
        lane = lax.broadcasted_iota(jnp.int32, (8, LANES), 1)
        tile = jnp.where(lane == k, high[rows], 0.0 if k == 0 else tile)
        tile = jnp.where(lane == LOW_LANE + k, place[rows] - high[rows] * LANES, tile)
    sent[2 * across * down] = tile.astype(jnp.bfloat16)

    def unitize_rows(normed, weight):
        embedded = jnp.dot(normed[...], weight[...], preferred_element_type=jnp.float32)
        squares = jnp.sum(embedded * embedded, axis=-1, keepdims=True) + 1e-06
        inverse = 1.0 / jnp.sqrt(squares)
        return embedded * inverse, inverse

    is_image = lax.axis_index("mod") == 0
    image_unit, image_inverse = unitize_rows(image_normed, image_weight)
    text_unit, text_inverse = unitize_rows(text_normed, text_weight)
    own = jnp.where(is_image, image_unit, text_unit)
    unit[...] = own
    other = jnp.where(is_image, text_unit, image_unit)
    for base, rows in ((0, own), (across * down, other)):
        for i in range(down):
            for k in range(across):
                tile = rows[i * 8 : i * 8 + 8, k * LANES : (k + 1) * LANES]
                sent[base + i * across + k] = tile.astype(jnp.bfloat16)
    side[...] = lane_table(
        {
            SIDE_INVERSE: jnp.where(is_image, image_inverse, text_inverse),
            SIDE_PLACE: place,
            SIDE_SCALE: spots[:, SIDE_SCALE : SIDE_SCALE + 1],
        },
        (row_count, LANES),
    )


def fold_rows(block, reduce):
    rows, lanes = block.shape
    if rows % 64 == 0:
        block = reduce(block.reshape(rows // 64, 64, lanes), axis=0)
    return reduce(block, axis=0, keepdims=True)


def score_kernel(order, own_all, other_all, digits, unit, side, loss_value, embed_grad, scores):
    row_count, width = unit.shape
    batch_total = own_all.shape[0]
    scale_value = side[0:1, SIDE_SCALE : SIDE_SCALE + 1]
    factor = scale_value * LOG2_E
    column = lax.broadcasted_iota(jnp.int32, (1, batch_total), 1).astype(jnp.float32)

    columns = digits[...].astype(jnp.float32)
    columns = columns * LANES + pltpu.roll(columns, LANES - LOW_LANE, axis=2)
    places = jnp.concatenate(
        [columns[i, :, k : k + 1] for i in range(len(order)) for k in range(row_count // 8)], axis=0
    )
    lanes = lax.broadcasted_iota(jnp.int32, (1, LANES), 1).astype(jnp.float32)
    row_tops = jnp.full((batch_total, LANES), -jnp.inf, jnp.float32)
    diagonal = jnp.zeros((batch_total, LANES), jnp.float32)
    column_lses = []
    for start in range(0, batch_total, CHUNK):
        count = min(CHUNK, batch_total - start)
        block = factor * lax.dot_general(
            own_all[...],
            other_all[start : start + count, :],
            (((1,), (1,)), ((), ())),
            preferred_element_type=jnp.float32,
        )
        scores[:, start : start + count] = block
        top = fold_rows(block, jnp.max)
        total = fold_rows(jnp.exp2(block - top), jnp.sum)
        column_lses.append(top + LOG2_E * jnp.log(total))
        for k in range(0, count, LANES):
            part = block[:, k : k + LANES]
            row_tops = jnp.maximum(row_tops, part)
            diagonal = jnp.where(places == lanes + (start + k), part, diagonal)
    column_lse = jnp.concatenate(column_lses, axis=1)
    mine = lax.axis_index("dp")
    first = jnp.int32(0)
    for here, sample in enumerate(order):
        first = jnp.where(mine == sample, here * row_count, first)
    block = scores[pl.ds(pl.multiple_of(first, 8), row_count), :]
    row_top = jnp.max(block, axis=1, keepdims=True)
    row_sum = jnp.sum(jnp.exp2(block - row_top), axis=1, keepdims=True)
    row_lse = row_top + LOG2_E * jnp.log(row_sum)
    matched = jnp.where(column == side[:, SIDE_PLACE : SIDE_PLACE + 1], 2.0, 0.0)
    pair_weight = jnp.exp2(block - row_lse) + jnp.exp2(block - column_lse) - matched
    unit_grad = (scale_value * (0.5 / batch_total)) * jnp.dot(
        pair_weight.astype(jnp.bfloat16),
        other_all[...],
        preferred_element_type=jnp.float32,
    )
    unit_rows = unit[...]
    along = jnp.sum(unit_rows * unit_grad, axis=-1, keepdims=True)
    embed_grad[0] = (unit_grad - unit_rows * along) * side[:, SIDE_INVERSE : SIDE_INVERSE + 1]

    row_top = jnp.max(row_tops, axis=1, keepdims=True)
    sums = jnp.zeros((batch_total, LANES), jnp.float32)
    for start in range(0, batch_total, LANES):
        sums = sums + jnp.exp2(scores[:, start : start + LANES] - row_top)
    row_lse = row_top + LOG2_E * jnp.log(jnp.sum(sums, axis=1, keepdims=True))
    total = jnp.sum(fold_rows(row_lse, jnp.sum)) + jnp.sum(column_lse) - 2.0 * jnp.sum(fold_rows(diagonal, jnp.sum))
    loss_value[0] = total * (float(np.log(2.0)) / (2.0 * batch_total))


def gather_both(
    order, image_pooled, text_pooled, image_gain, text_gain, image_proj, text_proj, logit_scale, pair_index
):
    row_count = image_pooled.shape[0]
    width = image_proj.shape[1]
    batch_total = row_count * len(order)
    f32, bf16 = jnp.float32, jnp.bfloat16
    tiles = row_count * width // (8 * LANES)
    operands = (image_pooled, text_pooled, image_gain, text_gain, pair_index)
    spread = pl.pallas_call(
        scale_kernel,
        out_shape=jax.ShapeDtypeStruct((8, LANES), f32),
        in_specs=[pl.BlockSpec(memory_space=pltpu.SMEM)],
        out_specs=pl.BlockSpec(memory_space=pltpu.VMEM),
        compiler_params=pltpu.CompilerParams(vmem_limit_bytes=KERNEL_BYTES),
        cost_estimate=pl.CostEstimate(flops=SCALE_COST, bytes_accessed=4_000_000, transcendentals=0),
        name="scale",
    )(logit_scale)
    image_normed, text_normed, spots = pl.pallas_call(
        lambda *refs: norm_kernel(order, *refs),
        out_shape=(
            jax.ShapeDtypeStruct(image_pooled.shape, bf16),
            jax.ShapeDtypeStruct(text_pooled.shape, bf16),
            jax.ShapeDtypeStruct((row_count, LANES), f32),
        ),
        in_specs=[pl.BlockSpec(memory_space=pltpu.VMEM)] * (1 + len(operands)),
        out_specs=[pl.BlockSpec(memory_space=pltpu.VMEM)] * 3,
        compiler_params=pltpu.CompilerParams(vmem_limit_bytes=KERNEL_BYTES),
        cost_estimate=pl.CostEstimate(flops=NORM_COST, bytes_accessed=4_000_000, transcendentals=0),
        name="norm",
    )(spread, *operands)
    sent, unit, side = pl.pallas_call(
        embed_kernel,
        out_shape=(
            jax.ShapeDtypeStruct((2 * tiles + 1, 8, LANES), bf16),
            jax.ShapeDtypeStruct((row_count, width), f32),
            jax.ShapeDtypeStruct((row_count, LANES), f32),
        ),
        in_specs=[pl.BlockSpec(memory_space=pltpu.VMEM)] * 5,
        out_specs=[pl.BlockSpec(memory_space=pltpu.VMEM)] * 3,
        compiler_params=pltpu.CompilerParams(vmem_limit_bytes=KERNEL_BYTES),
        name="embed",
    )(image_normed, text_normed, image_proj, text_proj, spots)
    every = lax.all_gather(
        sent.astype(jnp.float16), "dp", axis=0, tiled=True, axis_index_groups=[order]
    ).reshape(len(order), 2 * tiles + 1, 8, LANES)

    def plain(blocks):
        blocks = blocks.reshape(len(order), row_count // 8, width // LANES, 8, LANES)
        return blocks.transpose(0, 1, 3, 2, 4).reshape(batch_total, width).astype(bf16)

    own_all = plain(every[:, :tiles])
    other_all = plain(every[:, tiles : 2 * tiles])
    digits = every[:, 2 * tiles].astype(bf16)
    loss_value, embed_grad = pl.pallas_call(
        lambda *refs: score_kernel(order, *refs),
        out_shape=(
            jax.ShapeDtypeStruct((1,), f32),
            jax.ShapeDtypeStruct((1, row_count, width), f32),
        ),
        in_specs=[pl.BlockSpec(memory_space=pltpu.VMEM)] * 5,
        out_specs=[pl.BlockSpec(memory_space=pltpu.SMEM), pl.BlockSpec(memory_space=pltpu.VMEM)],
        scratch_shapes=[pltpu.VMEM((batch_total, batch_total), f32)],
        compiler_params=pltpu.CompilerParams(vmem_limit_bytes=KERNEL_BYTES),
        name="scores",
    )(own_all, other_all, digits, unit, side)
    return (loss_value[0], embed_grad)


def gather_one(
    image_pooled, text_pooled, image_gain, text_gain, image_proj, text_proj, logit_scale, pair_index
):
    module_index = lax.axis_index("mod")
    embedded = lax.cond(
        module_index == 0,
        lambda: normalize_project(image_pooled, image_gain, image_proj),
        lambda: normalize_project(text_pooled, text_gain, text_proj),
    )
    unit_rows, lengths = unitize(embedded)
    unit_half = unit_rows.astype(jnp.bfloat16)
    mirror_rows = from_partner(unit_half, "mod", 0)
    scale_value = logit_scale[0]
    row_count = unit_rows.shape[0]
    batch_total = row_count * lax.axis_size("dp")
    gathered = lax.all_gather(mirror_rows, "dp", axis=0, tiled=True)
    scores = similarity(unit_half, gathered, scale_value)
    own_lse = log_sum_exp(scores, 1)
    columns = lax.broadcasted_iota(jnp.int32, (row_count, batch_total), 1)
    matched = columns == pair_index[0][:, None]
    diagonal = jnp.sum(jnp.where(matched, scores, 0.0), axis=1)
    every_lse, every_diag = (
        lax.all_gather(own_lse, ("mod", "dp"), axis=0, tiled=True),
        lax.all_gather(diagonal, ("mod", "dp"), axis=0, tiled=True),
    )
    other_lse = lax.dynamic_slice_in_dim(every_lse, (1 - module_index) * batch_total, batch_total)
    loss_value = (jnp.sum(every_lse) - jnp.sum(every_diag)) / (2.0 * batch_total)
    pair_weight = (
        jnp.exp(scores - own_lse[:, None])
        + jnp.exp(scores - other_lse[None, :])
        - 2.0 * matched.astype(jnp.float32)
    ).astype(jnp.bfloat16)
    unit_grad = (
        scale_value
        / (2.0 * batch_total)
        * jnp.dot(pair_weight, gathered, preferred_element_type=jnp.float32)
    )
    embed_grad = (
        unit_grad - unit_rows * jnp.sum(unit_rows * unit_grad, axis=-1, keepdims=True)
    ) / lengths
    return (loss_value, embed_grad[None])


def solution(mesh):
    in_specs = (P("dp", None), P("dp", None), P(), P(), P(), P(), P(), P("mod", "dp"))
    out_specs = (P(), P("mod", "dp", None))
    order = closed_path(mesh)

    def local(*args):
        batch_total = args[0].shape[0] * lax.axis_size("dp")
        small = 4 * batch_total * batch_total <= SCORE_BYTES
        width = args[4].shape[1]
        if small and batch_total % LANES == 0 and args[0].shape[0] % 8 == 0 and width % LANES == 0:
            return gather_both(order, *args)
        return gather_one(*args)

    return jax.shard_map(local, mesh=mesh, in_specs=in_specs, out_specs=out_specs, check_vma=False)
```

```python
import jax
import jax.numpy as jnp
import numpy as np
from jax import lax
from jax.experimental import pallas as pl
from jax.experimental.pallas import tpu as pltpu
from jax.sharding import PartitionSpec as P

LANES = 128
SIDE_INVERSE, SIDE_PLACE, SIDE_SCALE = 0, 1, 2
LOW_LANE = 64
LOG2_E = float(np.log2(np.e))
CHUNK = 256
SCORE_BYTES = 2**22
KERNEL_BYTES = 2**24
NORM_COST = 1_000_000
IMAGE_COST = 1_000_000
SCALE_COST = 800_000_000


def closed_path(mesh):
    places = [getattr(d, "coords", None) for d in mesh.devices[0]]
    natural = list(range(len(places)))
    if any(p is None for p in places):
        return natural
    chips = {}
    for i, p in enumerate(places):
        chips.setdefault(tuple(p), []).append(i)
    span = [sorted({c[k] for c in chips}) for k in range(3)]
    wide = [k for k in range(3) if len(span[k]) > 1]
    if len(wide) != 2 or len(chips) != len(span[wide[0]]) * len(span[wide[1]]):
        return natural
    short, long = sorted(wide, key=lambda k: len(span[k]))
    if len(span[short]) != 2:
        return natural
    by = {(c[short], c[long]): v for c, v in chips.items()}
    there = [by[span[short][0], z] for z in span[long]]
    back = [by[span[short][1], z] for z in reversed(span[long])]
    return [i for cores in there + back for i in cores]


def from_partner(x, axis, bit):
    return lax.ppermute(x, axis, [(i, i ^ 1 << bit) for i in range(lax.axis_size(axis))])


def normalize_project(pooled, gain, weight):
    features = pooled.astype(jnp.float32)
    centered = features - jnp.mean(features, axis=-1, keepdims=True)
    variance = jnp.mean(centered * centered, axis=-1, keepdims=True)
    normalized = (centered * lax.rsqrt(variance + 1e-05) * gain).astype(jnp.bfloat16)
    return jnp.dot(normalized, weight, preferred_element_type=jnp.float32)


def unitize(embedded):
    lengths = jnp.sqrt(jnp.sum(embedded * embedded, axis=-1, keepdims=True) + 1e-06)
    return (embedded / lengths, lengths)


def similarity(left_rows, right_rows, scale_value):
    return scale_value * lax.dot_general(
        left_rows, right_rows, (((1,), (1,)), ((), ())), preferred_element_type=jnp.float32
    )


def log_sum_exp(scores, axis):
    top = jnp.max(scores, axis=axis)
    return top + jnp.log(jnp.sum(jnp.exp(scores - jnp.expand_dims(top, axis)), axis=axis))


def normalize(pooled, gain):
    features = pooled.astype(jnp.float32)
    centered = features - jnp.mean(features, axis=-1, keepdims=True)
    variance = jnp.mean(centered * centered, axis=-1, keepdims=True)
    return (centered * lax.rsqrt(variance + 1e-05) * gain).astype(jnp.bfloat16)


def lane_table(entries, shape):
    lane = lax.broadcasted_iota(jnp.int32, shape, 1)
    table = jnp.zeros(shape, jnp.float32)
    for i, entry in entries.items():
        table = jnp.where(lane == i, entry, table)
    return table


def scale_kernel(logit_scale, spread):
    spread[...] = jnp.full(spread.shape, logit_scale[0], jnp.float32)


def norm_kernel(
    order,
    spread,
    image_pooled,
    text_pooled,
    image_gain,
    text_gain,
    pair_index,
    image_normed,
    text_normed,
    side,
):
    row_count = image_pooled.shape[0]
    pairs = pair_index[...]
    places = pairs
    for here, sample in enumerate(order):
        inside = (pairs >= sample * row_count) & (pairs < (sample + 1) * row_count)
        places = jnp.where(inside, pairs + (here - sample) * row_count, places)
    square = (row_count, row_count)
    upright = lax.broadcasted_iota(jnp.int32, square, 0) == lax.broadcasted_iota(jnp.int32, square, 1)
    place = jnp.sum(jnp.where(upright, places.astype(jnp.float32), 0.0), axis=1, keepdims=True)
    shape = side.shape
    side[...] = lane_table({SIDE_PLACE: place, SIDE_SCALE: spread[0:1, 0:1]}, shape)
    image_normed[...] = normalize(image_pooled[...], image_gain[...][None, :])
    text_normed[...] = normalize(text_pooled[...], text_gain[...][None, :])


def unitize_rows(normed, weight):
    embedded = jnp.dot(normed, weight, preferred_element_type=jnp.float32)
    squares = jnp.sum(embedded * embedded, axis=-1, keepdims=True) + 1e-06
    inverse = 1.0 / jnp.sqrt(squares)
    return embedded * inverse, inverse


def image_kernel(normed, weight, unit, inverse):
    unit[...], scaling = unitize_rows(normed[...], weight[...])
    inverse[...] = jnp.broadcast_to(scaling, inverse.shape)


def embed_kernel(image_unit, image_inverse, text_normed, text_weight, spots, sent, unit, side):
    row_count, width = unit.shape
    place = spots[:, SIDE_PLACE : SIDE_PLACE + 1]
    high = jnp.floor(place * (1.0 / LANES))
    across, down = width // LANES, row_count // 8
    for k in range(down):
        rows = slice(k * 8, k * 8 + 8)
        lane = lax.broadcasted_iota(jnp.int32, (8, LANES), 1)
        tile = jnp.where(lane == k, high[rows], 0.0 if k == 0 else tile)
        tile = jnp.where(lane == LOW_LANE + k, place[rows] - high[rows] * LANES, tile)
    sent[2 * across * down] = tile.astype(jnp.bfloat16)

    is_image = lax.axis_index("mod") == 0
    text_unit, text_inverse = unitize_rows(text_normed[...], text_weight[...])
    own = jnp.where(is_image, image_unit[...], text_unit)
    unit[...] = own
    other = jnp.where(is_image, text_unit, image_unit[...])
    for base, rows in ((0, own), (across * down, other)):
        for i in range(down):
            for k in range(across):
                tile = rows[i * 8 : i * 8 + 8, k * LANES : (k + 1) * LANES]
                sent[base + i * across + k] = tile.astype(jnp.bfloat16)
    side[...] = lane_table(
        {
            SIDE_INVERSE: jnp.where(is_image, image_inverse[:, 0:1], text_inverse),
            SIDE_PLACE: place,
            SIDE_SCALE: spots[:, SIDE_SCALE : SIDE_SCALE + 1],
        },
        (row_count, LANES),
    )


def fold_rows(block, reduce):
    rows, lanes = block.shape
    if rows % 64 == 0:
        block = reduce(block.reshape(rows // 64, 64, lanes), axis=0)
    return reduce(block, axis=0, keepdims=True)


def score_kernel(order, own_all, other_all, digits, unit, side, loss_value, embed_grad, scores):
    row_count, width = unit.shape
    batch_total = own_all.shape[0]
    scale_value = side[0:1, SIDE_SCALE : SIDE_SCALE + 1]
    factor = scale_value * LOG2_E
    column = lax.broadcasted_iota(jnp.int32, (1, batch_total), 1).astype(jnp.float32)

    columns = digits[...].astype(jnp.float32)
    columns = columns * LANES + pltpu.roll(columns, LANES - LOW_LANE, axis=2)
    places = jnp.concatenate(
        [columns[i, :, k : k + 1] for i in range(len(order)) for k in range(row_count // 8)], axis=0
    )
    lanes = lax.broadcasted_iota(jnp.int32, (1, LANES), 1).astype(jnp.float32)
    row_tops = jnp.full((batch_total, LANES), -jnp.inf, jnp.float32)
    diagonal = jnp.zeros((batch_total, LANES), jnp.float32)
    column_lses = []
    for start in range(0, batch_total, CHUNK):
        count = min(CHUNK, batch_total - start)
        block = factor * lax.dot_general(
            own_all[...],
            other_all[start : start + count, :],
            (((1,), (1,)), ((), ())),
            preferred_element_type=jnp.float32,
        )
        scores[:, start : start + count] = block
        top = fold_rows(block, jnp.max)
        total = fold_rows(jnp.exp2(block - top), jnp.sum)
        column_lses.append(top + LOG2_E * jnp.log(total))
        for k in range(0, count, LANES):
            part = block[:, k : k + LANES]
            row_tops = jnp.maximum(row_tops, part)
            diagonal = jnp.where(places == lanes + (start + k), part, diagonal)
    column_lse = jnp.concatenate(column_lses, axis=1)
    mine = lax.axis_index("dp")
    first = jnp.int32(0)
    for here, sample in enumerate(order):
        first = jnp.where(mine == sample, here * row_count, first)
    block = scores[pl.ds(pl.multiple_of(first, 8), row_count), :]
    row_top = jnp.max(block, axis=1, keepdims=True)
    row_sum = jnp.sum(jnp.exp2(block - row_top), axis=1, keepdims=True)
    row_lse = row_top + LOG2_E * jnp.log(row_sum)
    matched = jnp.where(column == side[:, SIDE_PLACE : SIDE_PLACE + 1], 2.0, 0.0)
    pair_weight = jnp.exp2(block - row_lse) + jnp.exp2(block - column_lse) - matched
    unit_grad = (scale_value * (0.5 / batch_total)) * jnp.dot(
        pair_weight.astype(jnp.bfloat16),
        other_all[...],
        preferred_element_type=jnp.float32,
    )
    unit_rows = unit[...]
    along = jnp.sum(unit_rows * unit_grad, axis=-1, keepdims=True)
    embed_grad[0] = (unit_grad - unit_rows * along) * side[:, SIDE_INVERSE : SIDE_INVERSE + 1]

    row_top = jnp.max(row_tops, axis=1, keepdims=True)
    sums = jnp.zeros((batch_total, LANES), jnp.float32)
    for start in range(0, batch_total, LANES):
        sums = sums + jnp.exp2(scores[:, start : start + LANES] - row_top)
    row_lse = row_top + LOG2_E * jnp.log(jnp.sum(sums, axis=1, keepdims=True))
    total = jnp.sum(fold_rows(row_lse, jnp.sum)) + jnp.sum(column_lse) - 2.0 * jnp.sum(fold_rows(diagonal, jnp.sum))
    loss_value[0] = total * (float(np.log(2.0)) / (2.0 * batch_total))


def gather_both(
    order, image_pooled, text_pooled, image_gain, text_gain, image_proj, text_proj, logit_scale, pair_index
):
    row_count = image_pooled.shape[0]
    width = image_proj.shape[1]
    batch_total = row_count * len(order)
    f32, bf16 = jnp.float32, jnp.bfloat16
    tiles = row_count * width // (8 * LANES)
    operands = (image_pooled, text_pooled, image_gain, text_gain, pair_index)
    spread = pl.pallas_call(
        scale_kernel,
        out_shape=jax.ShapeDtypeStruct((8, LANES), f32),
        in_specs=[pl.BlockSpec(memory_space=pltpu.SMEM)],
        out_specs=pl.BlockSpec(memory_space=pltpu.VMEM),
        compiler_params=pltpu.CompilerParams(vmem_limit_bytes=KERNEL_BYTES),
        cost_estimate=pl.CostEstimate(flops=SCALE_COST, bytes_accessed=4_000_000, transcendentals=0),
        name="scale",
    )(logit_scale)
    image_normed, text_normed, spots = pl.pallas_call(
        lambda *refs: norm_kernel(order, *refs),
        out_shape=(
            jax.ShapeDtypeStruct(image_pooled.shape, bf16),
            jax.ShapeDtypeStruct(text_pooled.shape, bf16),
            jax.ShapeDtypeStruct((row_count, LANES), f32),
        ),
        in_specs=[pl.BlockSpec(memory_space=pltpu.VMEM)] * (1 + len(operands)),
        out_specs=[pl.BlockSpec(memory_space=pltpu.VMEM)] * 3,
        compiler_params=pltpu.CompilerParams(vmem_limit_bytes=KERNEL_BYTES),
        cost_estimate=pl.CostEstimate(flops=NORM_COST, bytes_accessed=4_000_000, transcendentals=0),
        name="norm",
    )(spread, *operands)
    image_unit, image_inverse = pl.pallas_call(
        image_kernel,
        out_shape=(
            jax.ShapeDtypeStruct((row_count, width), f32),
            jax.ShapeDtypeStruct((row_count, LANES), f32),
        ),
        in_specs=[pl.BlockSpec(memory_space=pltpu.VMEM)] * 2,
        out_specs=[pl.BlockSpec(memory_space=pltpu.VMEM)] * 2,
        compiler_params=pltpu.CompilerParams(vmem_limit_bytes=KERNEL_BYTES),
        cost_estimate=pl.CostEstimate(flops=IMAGE_COST, bytes_accessed=4_000_000, transcendentals=0),
        name="image",
    )(image_normed, image_proj)
    sent, unit, side = pl.pallas_call(
        embed_kernel,
        out_shape=(
            jax.ShapeDtypeStruct((2 * tiles + 1, 8, LANES), bf16),
            jax.ShapeDtypeStruct((row_count, width), f32),
            jax.ShapeDtypeStruct((row_count, LANES), f32),
        ),
        in_specs=[pl.BlockSpec(memory_space=pltpu.VMEM)] * 5,
        out_specs=[pl.BlockSpec(memory_space=pltpu.VMEM)] * 3,
        compiler_params=pltpu.CompilerParams(vmem_limit_bytes=KERNEL_BYTES),
        name="embed",
    )(image_unit, image_inverse, text_normed, text_proj, spots)
    every = lax.all_gather(
        sent.astype(jnp.float16), "dp", axis=0, tiled=True, axis_index_groups=[order]
    ).reshape(len(order), 2 * tiles + 1, 8, LANES)

    def plain(blocks):
        blocks = blocks.reshape(len(order), row_count // 8, width // LANES, 8, LANES)
        return blocks.transpose(0, 1, 3, 2, 4).reshape(batch_total, width).astype(bf16)

    own_all = plain(every[:, :tiles])
    other_all = plain(every[:, tiles : 2 * tiles])
    digits = every[:, 2 * tiles].astype(bf16)
    loss_value, embed_grad = pl.pallas_call(
        lambda *refs: score_kernel(order, *refs),
        out_shape=(
            jax.ShapeDtypeStruct((1,), f32),
            jax.ShapeDtypeStruct((1, row_count, width), f32),
        ),
        in_specs=[pl.BlockSpec(memory_space=pltpu.VMEM)] * 5,
        out_specs=[pl.BlockSpec(memory_space=pltpu.SMEM), pl.BlockSpec(memory_space=pltpu.VMEM)],
        scratch_shapes=[pltpu.VMEM((batch_total, batch_total), f32)],
        compiler_params=pltpu.CompilerParams(vmem_limit_bytes=KERNEL_BYTES),
        name="scores",
    )(own_all, other_all, digits, unit, side)
    return (loss_value[0], embed_grad)


def gather_one(
    image_pooled, text_pooled, image_gain, text_gain, image_proj, text_proj, logit_scale, pair_index
):
    module_index = lax.axis_index("mod")
    embedded = lax.cond(
        module_index == 0,
        lambda: normalize_project(image_pooled, image_gain, image_proj),
        lambda: normalize_project(text_pooled, text_gain, text_proj),
    )
    unit_rows, lengths = unitize(embedded)
    unit_half = unit_rows.astype(jnp.bfloat16)
    mirror_rows = from_partner(unit_half, "mod", 0)
    scale_value = logit_scale[0]
    row_count = unit_rows.shape[0]
    batch_total = row_count * lax.axis_size("dp")
    gathered = lax.all_gather(mirror_rows, "dp", axis=0, tiled=True)
    scores = similarity(unit_half, gathered, scale_value)
    own_lse = log_sum_exp(scores, 1)
    columns = lax.broadcasted_iota(jnp.int32, (row_count, batch_total), 1)
    matched = columns == pair_index[0][:, None]
    diagonal = jnp.sum(jnp.where(matched, scores, 0.0), axis=1)
    every_lse, every_diag = (
        lax.all_gather(own_lse, ("mod", "dp"), axis=0, tiled=True),
        lax.all_gather(diagonal, ("mod", "dp"), axis=0, tiled=True),
    )
    other_lse = lax.dynamic_slice_in_dim(every_lse, (1 - module_index) * batch_total, batch_total)
    loss_value = (jnp.sum(every_lse) - jnp.sum(every_diag)) / (2.0 * batch_total)
    pair_weight = (
        jnp.exp(scores - own_lse[:, None])
        + jnp.exp(scores - other_lse[None, :])
        - 2.0 * matched.astype(jnp.float32)
    ).astype(jnp.bfloat16)
    unit_grad = (
        scale_value
        / (2.0 * batch_total)
        * jnp.dot(pair_weight, gathered, preferred_element_type=jnp.float32)
    )
    embed_grad = (
        unit_grad - unit_rows * jnp.sum(unit_rows * unit_grad, axis=-1, keepdims=True)
    ) / lengths
    return (loss_value, embed_grad[None])


def solution(mesh):
    in_specs = (P("dp", None), P("dp", None), P(), P(), P(), P(), P(), P("mod", "dp"))
    out_specs = (P(), P("mod", "dp", None))
    order = closed_path(mesh)

    def local(*args):
        batch_total = args[0].shape[0] * lax.axis_size("dp")
        small = 4 * batch_total * batch_total <= SCORE_BYTES
        width = args[4].shape[1]
        if small and batch_total % LANES == 0 and args[0].shape[0] % 8 == 0 and width % LANES == 0:
            return gather_both(order, *args)
        return gather_one(*args)

    return jax.shard_map(local, mesh=mesh, in_specs=in_specs, out_specs=out_specs, check_vma=False)
```
